32 devices in a mesh: dp: 2 (over core), vocab: 16 (over z, y, x).
Axes of the slice: x: 2, y: 2, z: 4, core: 2. Of those that a mesh axis runs over, the one named last changes fastest.
Arguments:
- table: bfloat16 [16384, 4096], P('vocab'), may hold values from -0.75 to 0.75
- hidden: bfloat16 [512, 4096], P(('dp', 'vocab')), may hold values from -9 to 9
- cotangent: bfloat16 [512, 4096], P(('dp', 'vocab')), may hold values from -0.75 to 0.75
- input_ids: int32 [512], P('dp'), may hold values from 0 to 16383, as said below
- target_ids: int32 [512], P('dp'), may hold values from 0 to 16383
Outputs:
- table_grad: float32 [16384, 4096], P(('vocab', 'dp'))
- hidden_grad: bfloat16 [512, 4096], P(('dp', 'vocab'))
- token_loss: float32 [512], P('dp')
The draws below stay inside these ranges and needn't reach their ends.
Inputs may be any that keep to these rules, and one draw needn't show every extreme that they name: `input_ids`: the ids of one replica group may all lie in the 1024 rows of one index of vocab; in every draw some group's ids do.
All inputs are finite; a program needn't handle non-finite values.
Results may differ from the reference program's by a relative error of at most 0.0034.
Values may be sent and summed in bfloat16 or wider, within the bound.
A program may use at most 128 MiB of HBM per device.

```python
import jax
import jax.numpy as jnp
from jax import lax

D = 4096
V_DEV = 1024
MICRO = 8
MB_ROWS = 32
GROUP = 256
V = 16384
TOKENS = 512
N_DP = 2


def table_values(key):
    base = jax.random.normal(jax.random.fold_in(key, 11), (V, D), jnp.float32) * 0.125
    return jnp.clip(base, -0.75, 0.75)


def draw_table(key, part):
    return table_values(key).astype(jnp.bfloat16)


def draw_hidden(key, part):
    scales = jnp.exp(jax.random.uniform(jax.random.fold_in(key, 13), (TOKENS, 1), jnp.float32, jnp.log(0.12), jnp.log(0.5)))
    base = jax.random.normal(jax.random.fold_in(key, 12), (TOKENS, D), jnp.float32)
    return jnp.clip(base * scales, -8.0, 8.0).astype(jnp.bfloat16)


def draw_input_ids(key, part):
    groups = TOKENS // GROUP
    shards = V // V_DEV
    hot_group = jax.random.randint(jax.random.fold_in(key, 21), (), 0, groups)
    hot_shard = jax.random.randint(jax.random.fold_in(key, 22), (groups, 1), 0, shards)
    levels = jax.random.randint(jax.random.fold_in(key, 23), (groups, 1), 0, 5)
    group_index = jnp.arange(groups, dtype=jnp.int32)[:, None]
    levels = jnp.where(group_index == hot_group, 4, levels)
    pickers = jax.random.randint(jax.random.fold_in(key, 24), (groups, GROUP), 0, 4)
    concentrated = pickers < levels
    in_shard = hot_shard * V_DEV + jax.random.randint(jax.random.fold_in(key, 25), (groups, GROUP), 0, V_DEV)
    anywhere = jax.random.randint(jax.random.fold_in(key, 26), (groups, GROUP), 0, V)
    values = jnp.where(concentrated, in_shard, anywhere)
    return values.reshape(TOKENS).astype(jnp.int32)


def plant(values, stream_key, smallest, largest):
    shape = values.shape
    index_at = [jax.random.randint(jax.random.fold_in(stream_key, axis), (), 0, shape[axis]) for axis in range(len(shape))]
    values = values.at[tuple(index_at)].set(smallest)
    longest = shape.index(max(shape))
    index_at[longest] = (index_at[longest] + 1) % shape[longest]
    return values.at[tuple(index_at)].set(largest)


def shard_levels(own_key, dims, split, smallest, largest):
    def one(axis_at, parts):
        heights = jax.random.uniform(jax.random.fold_in(jax.random.fold_in(own_key, 6), axis_at), (parts,), jnp.float32, smallest / len(split), largest / len(split))
        return jnp.repeat(jnp.exp(heights), dims[axis_at] // parts).reshape((-1,) + (1,) * (len(dims) - axis_at - 1))

    loudness = one(*split[0])
    for cut in split[1:]:
        loudness = loudness * one(*cut)
    return loudness


def centred(stream_key, extent, deviation, reach, cuts=(), kind=jnp.bfloat16):
    values = jax.random.normal(stream_key, extent, jnp.float32) * deviation
    if len(cuts) > 0:
        values = shard_levels(stream_key, extent, cuts, -0.22, 0.18) * values
    return jnp.clip(values, min=-reach, max=reach).astype(kind)


def setup_inputs(seed: int = 0) -> dict:
    keys = jax.random.split(jax.random.key(seed), 6)
    return {
        "table": draw_table(jax.random.fold_in(keys[5], 71), 0),
        "hidden": draw_hidden(jax.random.fold_in(keys[5], 71), 0),
        "cotangent": centred(keys[2], (TOKENS, D), 0.05, 0.75, ((0, 32),)),
        "input_ids": draw_input_ids(jax.random.fold_in(keys[5], 71), 0),
        "target_ids": plant(jax.random.randint(keys[4], (TOKENS,), 0, V), jax.random.fold_in(keys[4], 1), 0, V - 1).astype(jnp.int32),
    }


def reference(table, hidden, cotangent, input_ids, target_ids):
    group = MICRO * MB_ROWS
    vocab_rows = table.shape[0]
    width = table.shape[1]
    columns = jnp.arange(vocab_rows, dtype=jnp.int32)

    def one_group(total, index):
        begin = (index * group).astype(jnp.int32)
        rows = lax.dynamic_slice_in_dim(hidden, begin, group, 0)
        incoming = lax.dynamic_slice_in_dim(cotangent, begin, group, 0)
        inputs = lax.dynamic_slice_in_dim(input_ids, begin, group, 0)
        targets = lax.dynamic_slice_in_dim(target_ids, begin, group, 0)
        logits = lax.dot_general(rows, table, (((1,), (1,)), ((), ())), preferred_element_type=jnp.float32)
        top = jnp.max(logits, axis=1)
        lse = top + jnp.log(jnp.sum(jnp.exp(logits - top[:, None]), axis=1))
        hit = targets[:, None] == columns[None, :]
        picked = jnp.sum(jnp.where(hit, logits, jnp.float32(0.0)), axis=1)
        loss = lse - picked
        probs = jnp.exp(logits - lse[:, None])
        dlogits = (probs - hit.astype(jnp.float32)).astype(jnp.bfloat16)
        row_grad = jnp.dot(dlogits, table, preferred_element_type=jnp.float32).astype(jnp.bfloat16)
        grad = lax.dot_general(dlogits, rows, (((0,), (0,)), ((), ())), preferred_element_type=jnp.float32)
        grad = grad.at[inputs].add(incoming.astype(jnp.float32))
        return total + grad, (row_grad, loss)

    start = jnp.zeros((vocab_rows, width), jnp.float32)
    total, (row_grads, losses) = lax.scan(one_group, start, jnp.arange(N_DP, dtype=jnp.int32))
    return total, row_grads.reshape(-1, width), losses.reshape(-1)
```

```python
import functools
import math

import jax
import jax.numpy as jnp
from jax import lax
from jax.experimental import pallas as pl
from jax.experimental.pallas import tpu as pltpu
from jax.sharding import PartitionSpec as P

MESH = pl.DeviceIdType.MESH
BF16 = jnp.bfloat16
F32 = jnp.float32
TILE = 512


def chunk_list(half):
    w = half // 4
    return [(i * w, w) for i in range(4)]


def count_copies(groups, n, chunks):
    nz = n // 4
    column = 3 + 2 * (nz - 1) + 2 * (nz - 2)
    first = 4 + 4 * (nz - 1) + 2 * (nz - 2)
    gather = 2 + first + 2 + 4 * (nz - 1) + 4 * column
    return 2 * gather + (n - 1) + 4 * (groups - 1) + chunks * (4 + 2 * (nz - 1))


def kernel(groups, n, table_hbm, hidden_hbm, cot_hbm, in_ids_hbm, tgt_hbm,
           tg_ref, hg_ref, loss_ref,
           table, x_all, logits, st, dl_ref, dlt_ref, e_in, hot, ids, tgt_ref,
           part, s1, r1, s2, r2, s3, r3, load_sem, send, recv):
    nz = n // 4
    rows, width = hg_ref.shape
    shard = table.shape[0]
    tokens = n * rows
    piece = shard // groups
    half = width // 2
    me = lax.axis_index("vocab")
    g = lax.axis_index("dp")
    z = me // 4
    y = (me % 4) // 2
    x = me % 2
    slots = iter(range(send.shape[0]))

    def at(zz, yy, xx):
        return zz * 4 + yy * 2 + xx

    x_peer = at(z, y, 1 - x)
    y_peer = at(z, 1 - y, x)
    above, below = z + 1 < nz, z > 0
    up, down = at(jnp.minimum(z + 1, nz - 1), y, x), at(jnp.maximum(z - 1, 0), y, x)

    def when(cond, act):
        if cond is None:
            act()
        else:
            pl.when(cond)(act)

    barrier = pltpu.get_barrier_semaphore()

    def greet(v, gg=None):
        pl.semaphore_signal(barrier, inc=1, device_id=(g if gg is None else gg, v), device_id_type=MESH)

    greet(x_peer)
    greet(y_peer)
    when(above, lambda: greet(up))
    when(below, lambda: greet(down))
    for d in range(1, groups):
        greet(me, (g + d) % groups)

    loads = [
        pltpu.make_async_copy(hidden_hbm, x_all.at[g, 0, me], load_sem.at[0]),
        pltpu.make_async_copy(cot_hbm, x_all.at[g, 1, me], load_sem.at[1]),
        pltpu.make_async_copy(in_ids_hbm, ids.at[0], load_sem.at[2]),
        pltpu.make_async_copy(tgt_hbm, tgt_ref, load_sem.at[3]),
        pltpu.make_async_copy(table_hbm, table, load_sem.at[4]),
    ]
    for c in loads:
        c.start()
    loads[0].wait()
    pl.semaphore_wait(barrier, 2 + above.astype(jnp.int32) + below.astype(jnp.int32) + groups - 1)

    started = []

    def both(a, b):
        return b if a is None else jnp.logical_and(a, b)

    def push(src, dst, v, gg=None, cond=None):
        k = next(slots)
        c = pltpu.make_async_remote_copy(
            src_ref=src, dst_ref=dst, send_sem=send.at[k], recv_sem=recv.at[k],
            device_id=(g if gg is None else gg, v), device_id_type=MESH)
        when(cond, c.start)
        started.append((cond, c))
        return c

    wa = width * 3 // 8
    wb = width * 5 // 16
    sets = [(0, wa), (wa, wb), (wa + wb, width - wa - wb)]

    class Column:
        def __init__(self, kind, k, yy, xx, fan):
            self.kind, self.cols, self.yy, self.xx, self.fan = kind, pl.ds(*sets[k]), yy, xx, fan
            mine = self.blk(z)
            self.ups = push(mine, mine, up, cond=above)
            self.downs = push(mine, mine, down, cond=below)
            self.seen = [(None, z, [push(mine, mine, p) for p in fan])]

        def blk(self, zz):
            return x_all.at[g, self.kind, at(zz, self.yy, self.xx), :, self.cols]

        def step(self, s):
            ups, downs = self.ups, self.downs
            for inward, cond, zz, go, nxt in ((ups, z - 1 - s >= 0, jnp.maximum(z - 1 - s, 0), above, up),
                                              (downs, z + 1 + s < nz, jnp.minimum(z + 1 + s, nz - 1), below, down)):
                when(cond, inward.wait_recv)
                b = self.blk(zz)
                if s < nz - 2:
                    c = push(b, b, nxt, cond=both(cond, go))
                    if nxt is up:
                        self.ups = c
                    else:
                        self.downs = c
                self.seen.append((cond, zz, [push(b, b, p, cond=cond) for p in self.fan]))

    finals = [[None] * 3, [None] * 3]

    def gather(kind):
        def own(k):
            return x_all.at[g, kind, me, :, pl.ds(*sets[k])]

        fb = push(own(1), own(1), x_peer)
        fc = push(own(2), own(2), y_peer)
        a = Column(kind, 0, y, x, [x_peer, y_peer])
        b1 = Column(kind, 1, y, x, [y_peer])
        c1 = Column(kind, 2, y, x, [x_peer])
        thirds = []

        def third(items):
            lo, span = sets[0]
            for cond, zz, (fx, fy) in items:
                when(cond, fx.wait_recv)
                b = x_all.at[g, kind, at(zz, y, 1 - x), :, pl.ds(lo, span // 2)]
                thirds.append((cond, push(b, b, y_peer, cond=cond)))
                when(cond, fy.wait_recv)
                b = x_all.at[g, kind, at(zz, 1 - y, x), :, pl.ds(lo + span // 2, span // 2)]
                thirds.append((cond, push(b, b, x_peer, cond=cond)))

        yield
        fb.wait_recv()
        b2 = Column(kind, 1, y, 1 - x, [y_peer])
        fc.wait_recv()
        c2 = Column(kind, 2, 1 - y, x, [x_peer])
        yield
        done = 0
        for s in range(nz - 1):
            new = len(a.seen)
            for col in (a, b1, c1, b2, c2):
                col.step(s)
            third(a.seen[done:new])
            done = new
            yield
        third(a.seen[done:])
        finals[kind] = [
            thirds,
            [(cond, c) for col in (b1, b2) for cond, _, cs in col.seen for c in cs],
            [(cond, c) for col in (c1, c2) for cond, _, cs in col.seen for c in cs],
        ]
        yield

    def land(kind, k):
        for cond, c in finals[kind][k]:
            when(cond, c.wait_recv)

    late = []

    def spread(kind):
        for d in range(1, groups):
            late.append(push(x_all.at[g, kind], x_all.at[g, kind], me, (g + d) % groups))

    g0 = gather(0)
    for _ in g0:
        pass
    loads[1].wait()
    g1 = gather(1)
    next(g1)

    offset = me * shard
    step = 256
    loads[4].wait()
    top = jnp.full((1, tokens), -jnp.inf, F32)
    for k in range(3):
        land(0, k)
        lo, span = sets[k]
        h = x_all[g, 0, :, :, lo:lo + span].reshape(tokens, span)
        for i in range(0, shard, step):
            lg = lax.dot_general(table[i:i + step, lo:lo + span], h, (((1,), (1,)), ((), ())),
                                 preferred_element_type=F32)
            if k > 0:
                lg = lg + logits[i:i + step]
            if k == 2:
                top = jnp.maximum(top, jnp.max(lg, axis=0, keepdims=True))
            logits[i:i + step] = lg
    loads[3].wait()
    total = jnp.zeros((1, tokens), F32)
    pick = jnp.zeros((1, tokens), F32)
    tgt = tgt_ref[...]
    for i in range(0, shard, step):
        lg = logits[i:i + step]
        vocab_row = offset + i + lax.broadcasted_iota(jnp.int32, (step, tokens), 0)
        total = total + jnp.sum(jnp.exp(lg - top), axis=0, keepdims=True)
        pick = pick + jnp.sum(jnp.where(vocab_row == tgt, lg, 0.0), axis=0, keepdims=True)
    line = lax.broadcasted_iota(jnp.int32, (4, tokens), 0)
    mine = jnp.where(line == 0, top, jnp.where(line == 1, total, pick))
    st[pl.ds(me, 1)] = mine[None]
    stats = [push(st.at[me], st.at[me], (me + d) % n) for d in range(1, n)]

    next(g1)
    spread(0)
    loads[2].wait()
    for d in range(1, groups):
        late.append(push(ids.at[0], ids.at[groups - d], me, (g + d) % groups))
    next(g1)

    for c in stats:
        c.wait_recv()
    top = st[0, 0:1]
    for j in range(1, n):
        top = jnp.maximum(top, st[j, 0:1])
    total = jnp.zeros((1, tokens), F32)
    pick = jnp.zeros((1, tokens), F32)
    for j in range(n):
        total = total + st[j, 1:2] * jnp.exp(st[j, 0:1] - top)
        pick = pick + st[j, 2:3]
    lse = top + jnp.log(total)
    loss_ref[...] = lse - pick
    for i in range(0, shard, step):
        vocab_row = offset + i + lax.broadcasted_iota(jnp.int32, (step, tokens), 0)
        hit = (vocab_row == tgt).astype(F32)
        d = (jnp.exp(logits[i:i + step] - lse) - hit).astype(BF16)
        dl_ref[i:i + step] = d
        dlt_ref[:, i:i + step] = d.T

    chunks = chunk_list(half)
    firsts, seconds, lasts = {}, {}, []

    def send_first(c):
        lo, wide = chunks[c]
        for side in range(2):
            base = side * half + lo
            p = jnp.dot(dlt_ref[...], table[:, base:base + wide], preferred_element_type=F32)
            part[:, :, :, :, base:base + wide] = p.reshape(nz, 2, 2, rows, wide)
            if side == 0:
                p = part[:, pl.ds(1 - y, 1), :, :, base:base + wide]
            else:
                p = part[:, :, pl.ds(1 - x, 1), :, base:base + wide]
            s1[side, :, :, :, lo:lo + wide] = p.reshape(nz, 2, rows, wide).astype(BF16)
            cols = pl.ds(lo, wide)
            firsts[side, c] = push(s1.at[side, :, :, :, cols], r1.at[side, :, :, :, cols],
                                   y_peer if side == 0 else x_peer)

    def merged_first(side, c, zz, yy, xx, count):
        lo, wide = chunks[c]
        base = side * half + lo
        a = part[pl.ds(zz, count), pl.ds(yy, 1), pl.ds(xx, 1), :, base:base + wide].reshape(count, rows, wide)
        b = r1[side, pl.ds(zz, count), pl.ds(xx if side == 0 else yy, 1), :, lo:lo + wide].reshape(count, rows, wide)
        return a + b.astype(F32)

    def send_second(c):
        lo, wide = chunks[c]
        for side in range(2):
            firsts[side, c].wait_recv()
            yy, xx, peer = (y, 1 - x, x_peer) if side == 0 else (1 - y, x, y_peer)
            s2[side, :, :, lo:lo + wide] = merged_first(side, c, 0, yy, xx, nz).astype(BF16)
            cols = pl.ds(lo, wide)
            seconds[side, c] = push(s2.at[side, :, :, cols], r2.at[side, :, :, cols], peer)

    def merged(side, c, zz):
        lo, wide = chunks[c]
        return (merged_first(side, c, zz, y, x, 1)
                + r2[side, pl.ds(zz, 1), :, lo:lo + wide].astype(F32)).reshape(rows, wide)

    def send_last(c):
        lo, wide = chunks[c]
        for side in range(2):
            seconds[side, c].wait_recv()
            for d in range(1, nz):
                zz = (z + d) % nz
                s3[side, d - 1, :, lo:lo + wide] = merged(side, c, zz).astype(BF16)
                cols = pl.ds(lo, wide)
                lasts.append((c, side, push(s3.at[side, d - 1, :, cols], r3.at[side, d - 1, :, cols], at(zz, y, x))))

    def tail(c):
        lo, wide = chunks[c]
        for side in range(2):
            for cc, ss, q in lasts:
                if (cc, ss) == (c, side):
                    q.wait_recv()
            acc = merged(side, c, z)
            for d in range(1, nz):
                acc = acc + r3[side, d - 1, :, lo:lo + wide].astype(F32)
            base = side * half + lo
            hg_ref[:, base:base + wide] = acc.astype(BF16)

    def send_dl():
        for d in range(1, groups):
            peer = (g + d) % groups
            late.append(push(dl_ref.at[pl.ds(pl.multiple_of(peer * piece, piece), piece)],
                             e_in.at[groups - d - 1], me, peer))

    def build_hot():
        line = me * shard + g * piece + lax.broadcasted_iota(jnp.int32, (piece, tokens), 0)
        for d in range(groups):
            hot[d] = (line == ids[d]).astype(F32).astype(BF16)

    def grad(t):
        cols = slice(t * TILE, (t + 1) * TILE)
        acc = jnp.dot(dl_ref[pl.ds(pl.multiple_of(g * piece, piece), piece)],
                      x_all[g, 0, :, :, cols].reshape(tokens, TILE), preferred_element_type=F32)
        acc = acc + jnp.dot(hot[0], x_all[g, 1, :, :, cols].reshape(tokens, TILE), preferred_element_type=F32)
        for d in range(1, groups):
            gg = (g + d) % groups
            acc = acc + jnp.dot(e_in[d - 1], x_all[gg, 0, :, :, cols].reshape(tokens, TILE),
                                preferred_element_type=F32)
            acc = acc + jnp.dot(hot[d], x_all[gg, 1, :, :, cols].reshape(tokens, TILE),
                                preferred_element_type=F32)
        tg_ref[:, cols] = acc

    tiles = width // TILE
    send_first(0)
    send_first(1)
    send_dl()
    next(g1)
    send_second(0)
    send_first(2)
    for _ in g1:
        pass
    send_second(1)
    send_first(3)
    send_last(0)
    send_second(2)
    for k in range(3):
        land(1, k)
    spread(1)
    send_last(1)
    send_second(3)
    for c in late:
        c.wait_recv()
    build_hot()
    send_last(2)
    for t in range(tiles // 2):
        grad(t)
    send_last(3)
    for t in range(tiles // 2, tiles):
        grad(t)
    for c in range(4):
        tail(c)
    for cond, c in started:
        when(cond, c.wait_send)


def write_kernel(tg_ref, hg_ref, loss_ref, tg_out, hg_out, loss_out, sem):
    width = tg_ref.shape[1]
    parts = tg_ref.shape[0] // 64
    copies = [pltpu.make_async_copy(hg_ref, hg_out, sem.at[0]), pltpu.make_async_copy(loss_ref, loss_out, sem.at[1])]
    for i in range(parts):
        r = pl.ds(i * 64, 64)
        copies.append(pltpu.make_async_copy(tg_ref.at[r], tg_out.at[r], sem.at[2 + i]))
    for c in copies:
        c.start()
    for c in copies:
        c.wait()


def solution(mesh):
    groups, n = mesh.shape["dp"], mesh.shape["vocab"]

    def body(table, hidden, cotangent, input_ids, target_ids):
        rows, width = hidden.shape
        shard = table.shape[0]
        nz = n // 4
        tokens = n * rows
        half = width // 2
        piece = shard // groups
        copies = count_copies(groups, n, len(chunk_list(half)))
        anys = pl.BlockSpec(memory_space=pl.ANY)
        vmem = pl.BlockSpec(memory_space=pltpu.VMEM)
        buffers = [
            pltpu.VMEM((shard, width), BF16),
            pltpu.VMEM((groups, 2, n, rows, width), BF16),
            pltpu.VMEM((shard, tokens), F32),
            pltpu.VMEM((n, 4, tokens), F32),
            pltpu.VMEM((shard, tokens), BF16),
            pltpu.VMEM((tokens, shard), BF16),
            pltpu.VMEM((groups - 1, piece, tokens), BF16),
            pltpu.VMEM((groups, piece, tokens), BF16),
            pltpu.VMEM((groups, 1, tokens), jnp.int32),
            pltpu.VMEM((1, tokens), jnp.int32),
            pltpu.VMEM((nz, 2, 2, rows, width), F32),
            pltpu.VMEM((2, nz, 2, rows, half), BF16),
            pltpu.VMEM((2, nz, 2, rows, half), BF16),
            pltpu.VMEM((2, nz, rows, half), BF16),
            pltpu.VMEM((2, nz, rows, half), BF16),
            pltpu.VMEM((2, nz - 1, rows, half), BF16),
            pltpu.VMEM((2, nz - 1, rows, half), BF16),
        ]
        used = sum(math.prod(b.shape) * jnp.dtype(b.dtype).itemsize for b in buffers)
        tg, hg, loss = pl.pallas_call(
            functools.partial(kernel, groups, n),
            out_shape=(
                pltpu.VMEM((piece, width), F32),
                pltpu.VMEM((rows, width), BF16),
                pltpu.VMEM((1, tokens), F32),
            ),
            in_specs=[anys] * 5,
            out_specs=(vmem, vmem, vmem),
            scratch_shapes=buffers + [
                pltpu.SemaphoreType.DMA((5,)),
                pltpu.SemaphoreType.DMA((copies,)),
                pltpu.SemaphoreType.DMA((copies,)),
            ],
            compiler_params=pltpu.CompilerParams(
                collective_id=0, has_side_effects=True, vmem_limit_bytes=used + 6 * 2**20),
        )(*(pltpu.with_memory_space_constraint(a, pltpu.HBM) for a in (
            table, hidden, cotangent, input_ids.reshape(1, tokens), target_ids.reshape(1, tokens))))
        tg = pltpu.with_memory_space_constraint(tg, pltpu.VMEM)
        hg = pltpu.with_memory_space_constraint(hg, pltpu.VMEM)
        loss = pltpu.with_memory_space_constraint(loss, pltpu.VMEM)
        table_grad, hg, loss = pl.pallas_call(
            write_kernel,
            out_shape=(
                jax.ShapeDtypeStruct((piece, width), F32),
                jax.ShapeDtypeStruct((rows, width), BF16),
                jax.ShapeDtypeStruct((1, tokens), F32),
            ),
            in_specs=[vmem] * 3,
            out_specs=(anys,) * 3,
            scratch_shapes=[pltpu.SemaphoreType.DMA((2 + piece // 64,))],
            compiler_params=pltpu.CompilerParams(vmem_limit_bytes=2 * 2**20),
        )(tg, hg, loss)
        return table_grad, hg, loss.reshape(tokens)

    return jax.shard_map(
        body,
        mesh=mesh,
        in_specs=(
            P("vocab", None),
            P(("dp", "vocab"), None),
            P(("dp", "vocab"), None),
            P("dp"),
            P("dp"),
        ),
        out_specs=(P(("vocab", "dp"), None), P(("dp", "vocab"), None), P("dp")),
        check_vma=False,
    )
```

```python
import functools
import math

import jax
import jax.numpy as jnp
from jax import lax
from jax.experimental import pallas as pl
from jax.experimental.pallas import tpu as pltpu
from jax.sharding import PartitionSpec as P

MESH = pl.DeviceIdType.MESH
BF16 = jnp.bfloat16
F32 = jnp.float32
TILE = 512
HIDDEN_A = 6
COT_A = 6


def chunk_list(half):
    eighth = half // 8
    spans, lo = [], 0
    for k in (2, 3, 2, 1):
        spans.append((lo, k * eighth))
        lo += k * eighth
    return spans


def count_semaphores(groups, n, chunks):
    nz = n // 4
    gather = 2 + 7 * nz + 3
    return 12 + 1 + 3 + 4 * (groups - 1), 2 * gather + 1 + 6 * chunks + 4 * (groups - 1)


def kernel(groups, n, table_hbm, hidden_hbm, cot_hbm, in_ids_hbm, tgt_hbm,
           tg_ref, hg_ref, loss_ref,
           table, x_all, logits, st, dl_ref, dlt_ref, e_in, hot, ids, tgt_ref,
           part, s1, r1, s2, r2, s3, r3, load_sem, send, recv):
    nz = n // 4
    rows, width = hg_ref.shape
    shard = table.shape[0]
    tokens = n * rows
    piece = shard // groups
    half = width // 2
    me = lax.axis_index("vocab")
    g = lax.axis_index("dp")
    z = me // 4
    y = (me % 4) // 2
    x = me % 2
    send_slots, recv_slots = iter(range(send.shape[0])), iter(range(recv.shape[0]))

    def at(zz, yy, xx):
        return zz * 4 + yy * 2 + xx

    x_peer = at(z, y, 1 - x)
    y_peer = at(z, 1 - y, x)
    above, below = z + 1 < nz, z > 0
    up, down = at(jnp.minimum(z + 1, nz - 1), y, x), at(jnp.maximum(z - 1, 0), y, x)

    def when(cond, act):
        if cond is None:
            act()
        else:
            pl.when(cond)(act)

    def every(cond, acts):
        def act():
            for one in acts:
                one()
        when(cond, act)

    barrier = pltpu.get_barrier_semaphore()

    def greet(v, gg=None):
        pl.semaphore_signal(barrier, inc=1, device_id=(g if gg is None else gg, v), device_id_type=MESH)

    greet(x_peer)
    greet(y_peer)
    when(above, lambda: greet(up))
    when(below, lambda: greet(down))
    for d in range(1, groups):
        greet(me, (g + d) % groups)

    loads = [
        pltpu.make_async_copy(hidden_hbm, x_all.at[g, 0, me], load_sem.at[0]),
        pltpu.make_async_copy(cot_hbm, x_all.at[g, 1, me], load_sem.at[1]),
        pltpu.make_async_copy(in_ids_hbm, ids.at[0], load_sem.at[2]),
        pltpu.make_async_copy(tgt_hbm, tgt_ref, load_sem.at[3]),
        pltpu.make_async_copy(table_hbm, table, load_sem.at[4]),
    ]
    for c in loads:
        c.start()
    loads[0].wait()
    pl.semaphore_wait(barrier, 2 + above.astype(jnp.int32) + below.astype(jnp.int32) + groups - 1)

    owed = []

    def push(src, dst, v, out, into, gg=None, cond=None, start=True):
        c = pltpu.make_async_remote_copy(
            src_ref=src, dst_ref=dst, send_sem=send.at[out], recv_sem=recv.at[into],
            device_id=(g if gg is None else gg, v), device_id_type=MESH)
        if start:
            when(cond, c.start)
        return c

    def drain():
        for cond, ref, out in owed:
            c = pltpu.make_async_remote_copy(
                src_ref=ref, dst_ref=ref, send_sem=send.at[out], recv_sem=recv.at[0],
                device_id=(g, me), device_id_type=MESH)
            when(cond, c.wait_send)
        owed.clear()

    def arrive(ref, into):
        pltpu.make_async_remote_copy(
            src_ref=ref, dst_ref=ref, send_sem=send.at[0], recv_sem=recv.at[into],
            device_id=(g, me), device_id_type=MESH).wait_recv()

    def take(it, count):
        return [next(it) for _ in range(count)][0]

    def split(k):
        wa = width * k // 16
        wb = (width - wa) // 2
        return [(0, wa), (wa, wb), (wa + wb, wb)]

    both = [split(HIDDEN_A), split(COT_A)]
    sets = both[0]
    inner = jnp.logical_and(above, below)
    outer = jnp.logical_not(inner)
    ways = []
    for s in range(nz - 1):
        lower, upper = z - 1 - s >= 0, z + 1 + s < nz
        ways.append(((lower, jnp.maximum(z - 1 - s, 0), above, up), (upper, jnp.minimum(z + 1 + s, nz - 1), below, down)))

    class Gather:
        def __init__(self, kind):
            self.kind, self.sets = kind, both[kind]
            self.swap_out, self.fan_a, self.fan_bc = (next(send_slots) for _ in range(3))
            self.line_out = [next(send_slots) for _ in range(3)]
            self.swap_in = [None, next(recv_slots), next(recv_slots)]
            self.full = [next(recv_slots) for _ in range(3)]
            self.via = {0: take(recv_slots, nz), 1: take(recv_slots, nz)}

            def some(k, count):
                return x_all.at[g, kind, pl.ds(0, count), :, pl.ds(*self.sets[k])]

            self.some = some
            self.columns = {}

        def owe(self):
            owed.append((None, self.some(1, 1), self.swap_out))
            owed.append((None, self.some(2, 1), self.swap_out))
            owed.append((None, self.some(0, 3 * nz), self.fan_a))
            owed.append((None, self.some(1, 2 * nz), self.fan_bc))
            owed.append((None, self.some(2, 2 * nz), self.fan_bc))
            for k in range(3):
                lines = 1 if k == 0 else 2
                owed.append((inner, self.some(k, lines * (nz + 1)), self.line_out[k]))
                owed.append((outer, self.some(k, lines), self.line_out[k]))

        def blk(self, k, zz, yy, xx):
            return x_all.at[g, self.kind, at(zz, yy, xx), :, pl.ds(*self.sets[k])]

        def swap(self):
            for k, peer in ((1, x_peer), (2, y_peer)):
                b = self.blk(k, z, y, x)
                push(b, b, peer, self.swap_out, self.swap_in[k])

        def line(self, name, k, yy, xx):
            base = take(recv_slots, nz)
            self.columns[name] = (k, yy, xx, base)
            b = self.blk(k, z, yy, xx)
            push(b, b, up, self.line_out[k], base + z, cond=above)
            push(b, b, down, self.line_out[k], base + z, cond=below)

        def lines1(self):
            self.line("a", 0, y, x)
            self.line("b1", 1, y, x)
            self.line("c1", 2, y, x)

        def lines2(self):
            arrive(self.blk(1, z, y, x), self.swap_in[1])
            self.line("b2", 1, y, 1 - x)
            arrive(self.blk(2, z, y, x), self.swap_in[2])
            self.line("c2", 2, 1 - y, x)

        def fans(self, name, zz):
            k, yy, xx, _ = self.columns[name]
            b = self.blk(k, zz, yy, xx)
            if k == 0:
                return [push(b, b, x_peer, self.fan_a, self.via[0] + zz, start=False),
                        push(b, b, y_peer, self.fan_a, self.via[1] + zz, start=False)]
            return [push(b, b, y_peer if k == 1 else x_peer, self.fan_bc, self.full[k], start=False)]

        def share(self, *names):
            for name in names:
                for c in self.fans(name, z):
                    c.start()

        def step(self, s, *names):
            for name in names:
                k, yy, xx, base = self.columns[name]
                for cond, zz, go, nxt in ways[s]:
                    b = self.blk(k, zz, yy, xx)
                    relay = push(b, b, nxt, self.line_out[k], base + zz, start=False)
                    fans = self.fans(name, zz)

                    def act():
                        relay.wait_recv()
                        if s < nz - 2:
                            pl.when(go)(relay.start)
                        for c in fans:
                            c.start()

                    pl.when(cond)(act)

        def third(self, s):
            lo, span = self.sets[0]
            for cond, zz in [(None, z)] if s < 0 else [(w[0], w[1]) for w in ways[s]]:
                full = self.blk(0, zz, y, x)
                b = x_all.at[g, self.kind, at(zz, y, 1 - x), :, pl.ds(lo, span // 2)]
                tx = push(b, b, y_peer, self.fan_a, self.full[0], start=False)
                b = x_all.at[g, self.kind, at(zz, 1 - y, x), :, pl.ds(lo + span // 2, span // 2)]
                ty = push(b, b, x_peer, self.fan_a, self.full[0], start=False)

                def act():
                    arrive(full, self.via[0] + zz)
                    tx.start()
                    arrive(full, self.via[1] + zz)
                    ty.start()

                when(cond, act)

        def land(self, k):
            arrive(self.some(k, nz if k == 0 else 2 * nz), self.full[k])

    late = []

    def lone(src, dst, gg):
        k = next(send_slots)
        owed.append((None, src, k))
        return push(src, dst, me, k, next(recv_slots), gg)

    def spread(kind):
        for d in range(1, groups):
            late.append(lone(x_all.at[g, kind], x_all.at[g, kind], (g + d) % groups))

    g0, g1 = Gather(0), Gather(1)
    g0.swap()
    g0.lines1()
    g0.share("a", "b1", "c1")
    g0.lines2()
    g0.share("b2", "c2")
    loads[1].wait()
    g1.swap()
    for s in range(nz - 2):
        g0.step(s, "a")
        g0.third(s - 1)
        g0.step(s, "b1", "c1", "b2", "c2")
    g1.lines1()
    g1.lines2()
    g0.step(nz - 2, "a")
    g0.third(nz - 3)
    g0.step(nz - 2, "b1", "c1")
    g0.third(nz - 2)
    g0.step(nz - 2, "b2", "c2")
    g0.owe()
    g1.share("a", "b1", "c1", "b2", "c2")

    offset = me * shard
    step = 256
    loads[4].wait()
    top = jnp.full((1, tokens), -jnp.inf, F32)
    for k in range(3):
        with jax.named_scope('land'):
            g0.land(k)
        lo, span = sets[k]
        h = x_all[g, 0, :, :, lo:lo + span].reshape(tokens, span)
        for i in range(0, shard, step):
            lg = lax.dot_general(table[i:i + step, lo:lo + span], h, (((1,), (1,)), ((), ())),
                                 preferred_element_type=F32)
            if k > 0:
                lg = lg + logits[i:i + step]
            if k == 2:
                top = jnp.maximum(top, jnp.max(lg, axis=0, keepdims=True))
            logits[i:i + step] = lg
    g1.step(0, "a")
    g1.third(-1)
    g1.step(0, "b1", "c1", "b2", "c2")
    loads[3].wait()
    total = jnp.zeros((1, tokens), F32)
    pick = jnp.zeros((1, tokens), F32)
    tgt = tgt_ref[...]
    for i in range(0, shard, step):
        lg = logits[i:i + step]
        vocab_row = offset + i + lax.broadcasted_iota(jnp.int32, (step, tokens), 0)
        total = total + jnp.sum(jnp.exp(lg - top), axis=0, keepdims=True)
        pick = pick + jnp.sum(jnp.where(vocab_row == tgt, lg, 0.0), axis=0, keepdims=True)
    line = lax.broadcasted_iota(jnp.int32, (4, tokens), 0)
    mine = jnp.where(line == 0, top, jnp.where(line == 1, total, pick))
    st[pl.ds(me, 1)] = mine[None]
    stat_out, stat_in = next(send_slots), next(recv_slots)
    for d in range(1, n):
        push(st.at[me], st.at[me], (me + d) % n, stat_out, stat_in)
    owed.append((None, st.at[pl.ds(0, n - 1)], stat_out))

    spread(0)
    loads[2].wait()
    for d in range(1, groups):
        late.append(lone(ids.at[0], ids.at[groups - d], (g + d) % groups))
    for s in range(1, nz - 2):
        g1.step(s, "a")
        g1.third(s - 1)
        g1.step(s, "b1", "c1", "b2", "c2")
    arrive(st.at[pl.ds(0, n - 1)], stat_in)
    top = st[0, 0:1]
    for j in range(1, n):
        top = jnp.maximum(top, st[j, 0:1])
    total = jnp.zeros((1, tokens), F32)
    pick = jnp.zeros((1, tokens), F32)
    for j in range(n):
        total = total + st[j, 1:2] * jnp.exp(st[j, 0:1] - top)
        pick = pick + st[j, 2:3]
    lse = top + jnp.log(total)
    loss_ref[...] = lse - pick
    for i in range(0, shard, step):
        vocab_row = offset + i + lax.broadcasted_iota(jnp.int32, (step, tokens), 0)
        hit = (vocab_row == tgt).astype(F32)
        d = (jnp.exp(logits[i:i + step] - lse) - hit).astype(BF16)
        dl_ref[i:i + step] = d
        dlt_ref[:, i:i + step] = d.T

    chunks = chunk_list(half)
    outs = [next(send_slots) for _ in range(3)]
    owed.extend([(None, s1, outs[0]), (None, s2, outs[1]), (None, s3, outs[2])])
    ins = {(stage, side, c): next(recv_slots) for stage in range(3) for side in range(2) for c in range(len(chunks))}

    def send_first(c):
        lo, wide = chunks[c]
        for side in range(2):
            base = side * half + lo
            p = jnp.dot(dlt_ref[...], table[:, base:base + wide], preferred_element_type=F32)
            part[:, :, :, :, base:base + wide] = p.reshape(nz, 2, 2, rows, wide)
            if side == 0:
                p = part[:, pl.ds(1 - y, 1), :, :, base:base + wide]
            else:
                p = part[:, :, pl.ds(1 - x, 1), :, base:base + wide]
            s1[side, :, :, :, lo:lo + wide] = p.reshape(nz, 2, rows, wide).astype(BF16)
            cols = pl.ds(lo, wide)
            push(s1.at[side, :, :, :, cols], r1.at[side, :, :, :, cols],
                 y_peer if side == 0 else x_peer, outs[0], ins[0, side, c])

    def merged_first(side, c, zz, yy, xx, count):
        lo, wide = chunks[c]
        base = side * half + lo
        a = part[pl.ds(zz, count), pl.ds(yy, 1), pl.ds(xx, 1), :, base:base + wide].reshape(count, rows, wide)
        b = r1[side, pl.ds(zz, count), pl.ds(xx if side == 0 else yy, 1), :, lo:lo + wide].reshape(count, rows, wide)
        return a + b.astype(F32)

    def send_second(c):
        lo, wide = chunks[c]
        for side in range(2):
            arrive(r1.at[side, :, :, :, pl.ds(lo, wide)], ins[0, side, c])
            yy, xx, peer = (y, 1 - x, x_peer) if side == 0 else (1 - y, x, y_peer)
            s2[side, :, :, lo:lo + wide] = merged_first(side, c, 0, yy, xx, nz).astype(BF16)
            cols = pl.ds(lo, wide)
            push(s2.at[side, :, :, cols], r2.at[side, :, :, cols], peer, outs[1], ins[1, side, c])

    def merged(side, c, zz):
        lo, wide = chunks[c]
        return (merged_first(side, c, zz, y, x, 1)
                + r2[side, pl.ds(zz, 1), :, lo:lo + wide].astype(F32)).reshape(rows, wide)

    def send_last(c):
        lo, wide = chunks[c]
        for side in range(2):
            arrive(r2.at[side, :, :, pl.ds(lo, wide)], ins[1, side, c])
            for d in range(1, nz):
                zz = (z + d) % nz
                s3[side, d - 1, :, lo:lo + wide] = merged(side, c, zz).astype(BF16)
                cols = pl.ds(lo, wide)
                push(s3.at[side, d - 1, :, cols], r3.at[side, d - 1, :, cols], at(zz, y, x), outs[2], ins[2, side, c])

    def tail(c):
        lo, wide = chunks[c]
        for side in range(2):
            arrive(r3.at[side, :, :, pl.ds(lo, wide)], ins[2, side, c])
            acc = merged(side, c, z)
            for d in range(1, nz):
                acc = acc + r3[side, d - 1, :, lo:lo + wide].astype(F32)
            base = side * half + lo
            hg_ref[:, base:base + wide] = acc.astype(BF16)

    def send_dl():
        for d in range(1, groups):
            peer = (g + d) % groups
            late.append(lone(dl_ref.at[pl.ds(pl.multiple_of(peer * piece, piece), piece)],
                             e_in.at[groups - d - 1], peer))

    def build_hot():
        line = me * shard + g * piece + lax.broadcasted_iota(jnp.int32, (piece, tokens), 0)
        for d in range(groups):
            hot[d] = (line == ids[d]).astype(F32).astype(BF16)

    def settle():
        for c in late:
            c.wait_recv()
        late.clear()

    def grad(t, kind):
        cols = slice(t * TILE, (t + 1) * TILE)
        acc = None
        for d in range(groups):
            if kind == 1:
                e = hot[d]
            elif d == 0:
                e = dl_ref[pl.ds(pl.multiple_of(g * piece, piece), piece)]
            else:
                e = e_in[d - 1]
            p = jnp.dot(e, x_all[(g + d) % groups, kind, :, :, cols].reshape(tokens, TILE),
                        preferred_element_type=F32)
            acc = p if acc is None else acc + p
        if kind == 1:
            acc = acc + tg_ref[:, cols]
        tg_ref[:, cols] = acc

    tiles = width // TILE
    send_first(0)
    send_dl()
    send_first(1)
    settle()
    build_hot()
    for t in range(tiles):
        grad(t, 0)
    g1.step(nz - 2, "a")
    g1.third(nz - 3)
    g1.step(nz - 2, "b1", "c1")
    g1.third(nz - 2)
    g1.step(nz - 2, "b2", "c2")
    g1.owe()
    send_second(0)
    send_first(2)
    send_second(1)
    send_last(0)
    send_first(3)
    for k in range(3):
        g1.land(k)
    spread(1)
    send_second(2)
    send_last(1)
    send_second(3)
    send_last(2)
    send_last(3)
    settle()
    for t in range(tiles):
        grad(t, 1)
    drain()
    for c in range(len(chunks)):
        tail(c)


def write_kernel(tg_ref, hg_ref, loss_ref, tg_out, hg_out, loss_out, sem):
    width = tg_ref.shape[1]
    parts = tg_ref.shape[0] // 64
    copies = [pltpu.make_async_copy(hg_ref, hg_out, sem.at[0]), pltpu.make_async_copy(loss_ref, loss_out, sem.at[1])]
    for i in range(parts):
        r = pl.ds(i * 64, 64)
        copies.append(pltpu.make_async_copy(tg_ref.at[r], tg_out.at[r], sem.at[2 + i]))
    for c in copies:
        c.start()
    for c in copies:
        c.wait()


def solution(mesh):
    groups, n = mesh.shape["dp"], mesh.shape["vocab"]

    def body(table, hidden, cotangent, input_ids, target_ids):
        rows, width = hidden.shape
        shard = table.shape[0]
        nz = n // 4
        tokens = n * rows
        half = width // 2
        piece = shard // groups
        sends, recvs = count_semaphores(groups, n, len(chunk_list(half)))
        anys = pl.BlockSpec(memory_space=pl.ANY)
        vmem = pl.BlockSpec(memory_space=pltpu.VMEM)
        buffers = [
            pltpu.VMEM((shard, width), BF16),
            pltpu.VMEM((groups, 2, n, rows, width), BF16),
            pltpu.VMEM((shard, tokens), F32),
            pltpu.VMEM((n, 4, tokens), F32),
            pltpu.VMEM((shard, tokens), BF16),
            pltpu.VMEM((tokens, shard), BF16),
            pltpu.VMEM((groups - 1, piece, tokens), BF16),
            pltpu.VMEM((groups, piece, tokens), BF16),
            pltpu.VMEM((groups, 1, tokens), jnp.int32),
            pltpu.VMEM((1, tokens), jnp.int32),
            pltpu.VMEM((nz, 2, 2, rows, width), F32),
            pltpu.VMEM((2, nz, 2, rows, half), BF16),
            pltpu.VMEM((2, nz, 2, rows, half), BF16),
            pltpu.VMEM((2, nz, rows, half), BF16),
            pltpu.VMEM((2, nz, rows, half), BF16),
            pltpu.VMEM((2, nz - 1, rows, half), BF16),
            pltpu.VMEM((2, nz - 1, rows, half), BF16),
        ]
        used = sum(math.prod(b.shape) * jnp.dtype(b.dtype).itemsize for b in buffers)
        tg, hg, loss = pl.pallas_call(
            functools.partial(kernel, groups, n),
            out_shape=(
                pltpu.VMEM((piece, width), F32),
                pltpu.VMEM((rows, width), BF16),
                pltpu.VMEM((1, tokens), F32),
            ),
            in_specs=[anys] * 5,
            out_specs=(vmem, vmem, vmem),
            scratch_shapes=buffers + [
                pltpu.SemaphoreType.DMA((5,)),
                pltpu.SemaphoreType.DMA((sends,)),
                pltpu.SemaphoreType.DMA((recvs,)),
            ],
            compiler_params=pltpu.CompilerParams(
                collective_id=0, has_side_effects=True, vmem_limit_bytes=used + 6 * 2**20),
        )(*(pltpu.with_memory_space_constraint(a, pltpu.HBM) for a in (
            table, hidden, cotangent, input_ids.reshape(1, tokens), target_ids.reshape(1, tokens))))
        tg = pltpu.with_memory_space_constraint(tg, pltpu.VMEM)
        hg = pltpu.with_memory_space_constraint(hg, pltpu.VMEM)
        loss = pltpu.with_memory_space_constraint(loss, pltpu.VMEM)
        table_grad, hg, loss = pl.pallas_call(
            write_kernel,
            out_shape=(
                jax.ShapeDtypeStruct((piece, width), F32),
                jax.ShapeDtypeStruct((rows, width), BF16),
                jax.ShapeDtypeStruct((1, tokens), F32),
            ),
            in_specs=[vmem] * 3,
            out_specs=(anys,) * 3,
            scratch_shapes=[pltpu.SemaphoreType.DMA((2 + piece // 64,))],
            compiler_params=pltpu.CompilerParams(vmem_limit_bytes=2 * 2**20),
        )(tg, hg, loss)
        return table_grad, hg, loss.reshape(tokens)

    return jax.shard_map(
        body,
        mesh=mesh,
        in_specs=(
            P("vocab", None),
            P(("dp", "vocab"), None),
            P(("dp", "vocab"), None),
            P("dp"),
            P("dp"),
        ),
        out_specs=(P(("vocab", "dp"), None), P(("dp", "vocab"), None), P("dp")),
        check_vma=False,
    )
```

```python
import functools
import math

import jax
import jax.numpy as jnp
from jax import lax
from jax.experimental import pallas as pl
from jax.experimental.pallas import tpu as pltpu
from jax.sharding import PartitionSpec as P

MESH = pl.DeviceIdType.MESH
BF16 = jnp.bfloat16
F32 = jnp.float32
TILE = 512
HIDDEN_A = 6
COT_A = 6


def chunk_list(half):
    eighth = half // 8
    spans, lo = [], 0
    for k in (2, 3, 2, 1):
        spans.append((lo, k * eighth))
        lo += k * eighth
    return spans


def count_semaphores(groups, n, chunks):
    nz = n // 4
    gather = 2 + 7 * nz + 3
    return 12 + 1 + 3 + 4 * (groups - 1), 2 * gather + 1 + 6 * chunks + 4 * (groups - 1)


def kernel(groups, n, table_hbm, hidden_hbm, cot_hbm, in_ids_hbm, tgt_hbm,
           tg_ref, hg_ref, loss_ref,
           table, x_all, logits, st, dl_ref, dlt_ref, e_in, hot, ids, tgt_ref,
           part, s1, r1, s2, r2, s3, r3, load_sem, send, recv):
    nz = n // 4
    rows, width = hg_ref.shape
    shard = table.shape[0]
    tokens = n * rows
    piece = shard // groups
    half = width // 2
    me = lax.axis_index("vocab")
    g = lax.axis_index("dp")
    z = me // 4
    y = (me % 4) // 2
    x = me % 2
    send_slots, recv_slots = iter(range(send.shape[0])), iter(range(recv.shape[0]))

    def at(zz, yy, xx):
        return zz * 4 + yy * 2 + xx

    x_peer = at(z, y, 1 - x)
    y_peer = at(z, 1 - y, x)
    above, below = z + 1 < nz, z > 0
    up, down = at(jnp.minimum(z + 1, nz - 1), y, x), at(jnp.maximum(z - 1, 0), y, x)

    def when(cond, act):
        if cond is None:
            act()
        else:
            pl.when(cond)(act)

    def every(cond, acts):
        def act():
            for one in acts:
                one()
        when(cond, act)

    barrier = pltpu.get_barrier_semaphore()

    def greet(v, gg=None):
        pl.semaphore_signal(barrier, inc=1, device_id=(g if gg is None else gg, v), device_id_type=MESH)

    greet(x_peer)
    greet(y_peer)
    when(above, lambda: greet(up))
    when(below, lambda: greet(down))
    for d in range(1, groups):
        greet(me, (g + d) % groups)

    loads = [
        pltpu.make_async_copy(hidden_hbm, x_all.at[g, 0, me], load_sem.at[0]),
        pltpu.make_async_copy(cot_hbm, x_all.at[g, 1, me], load_sem.at[1]),
        pltpu.make_async_copy(in_ids_hbm, ids.at[0], load_sem.at[2]),
        pltpu.make_async_copy(tgt_hbm, tgt_ref, load_sem.at[3]),
        pltpu.make_async_copy(table_hbm, table, load_sem.at[4]),
    ]
    for c in loads:
        c.start()
    loads[0].wait()
    pl.semaphore_wait(barrier, 2 + above.astype(jnp.int32) + below.astype(jnp.int32) + groups - 1)

    owed = []

    def push(src, dst, v, out, into, gg=None, cond=None, start=True):
        c = pltpu.make_async_remote_copy(
            src_ref=src, dst_ref=dst, send_sem=send.at[out], recv_sem=recv.at[into],
            device_id=(g if gg is None else gg, v), device_id_type=MESH)
        if start:
            when(cond, c.start)
        return c

    def drain():
        for cond, ref, out in owed:
            c = pltpu.make_async_remote_copy(
                src_ref=ref, dst_ref=ref, send_sem=send.at[out], recv_sem=recv.at[0],
                device_id=(g, me), device_id_type=MESH)
            when(cond, c.wait_send)
        owed.clear()

    def arrive(ref, into):
        pltpu.make_async_remote_copy(
            src_ref=ref, dst_ref=ref, send_sem=send.at[0], recv_sem=recv.at[into],
            device_id=(g, me), device_id_type=MESH).wait_recv()

    def take(it, count):
        return [next(it) for _ in range(count)][0]

    def split(k):
        wa = width * k // 16
        wb = (width - wa) // 2
        return [(0, wa), (wa, wb), (wa + wb, wb)]

    both = [split(HIDDEN_A), split(COT_A)]
    sets = both[0]
    inner = jnp.logical_and(above, below)
    outer = jnp.logical_not(inner)
    ways = []
    for s in range(nz - 1):
        lower, upper = z - 1 - s >= 0, z + 1 + s < nz
        ways.append(((lower, jnp.maximum(z - 1 - s, 0), above, up), (upper, jnp.minimum(z + 1 + s, nz - 1), below, down)))

    class Gather:
        def __init__(self, kind):
            self.kind, self.sets = kind, both[kind]
            self.swap_out, self.fan_a, self.fan_bc = (next(send_slots) for _ in range(3))
            self.line_out = [next(send_slots) for _ in range(3)]
            self.swap_in = [None, next(recv_slots), next(recv_slots)]
            self.full = [next(recv_slots) for _ in range(3)]
            self.via = {0: take(recv_slots, nz), 1: take(recv_slots, nz)}

            def some(k, count):
                return x_all.at[g, kind, pl.ds(0, count), :, pl.ds(*self.sets[k])]

            self.some = some
            self.columns = {}

        def owe(self):
            owed.append((None, self.some(1, 1), self.swap_out))
            owed.append((None, self.some(2, 1), self.swap_out))
            owed.append((None, self.some(0, 3 * nz), self.fan_a))
            owed.append((None, self.some(1, 2 * nz), self.fan_bc))
            owed.append((None, self.some(2, 2 * nz), self.fan_bc))
            for k in range(3):
                lines = 1 if k == 0 else 2
                owed.append((inner, self.some(k, lines * (nz + 1)), self.line_out[k]))
                owed.append((outer, self.some(k, lines), self.line_out[k]))

        def blk(self, k, zz, yy, xx):
            return x_all.at[g, self.kind, at(zz, yy, xx), :, pl.ds(*self.sets[k])]

        def swap(self):
            for k, peer in ((1, x_peer), (2, y_peer)):
                b = self.blk(k, z, y, x)
                push(b, b, peer, self.swap_out, self.swap_in[k])

        def register(self):
            for name, k, yy, xx in (("a", 0, y, x), ("b1", 1, y, x), ("c1", 2, y, x),
                                    ("b2", 1, y, 1 - x), ("c2", 2, 1 - y, x)):
                self.columns[name] = (k, yy, xx, take(recv_slots, nz))

        def line(self, name):
            k, yy, xx, base = self.columns[name]
            b = self.blk(k, z, yy, xx)
            push(b, b, up, self.line_out[k], base + z, cond=above)
            push(b, b, down, self.line_out[k], base + z, cond=below)

        def lines1(self):
            self.line("a")
            self.line("b1")
            self.line("c1")

        def lines2(self):
            arrive(self.blk(1, z, y, x), self.swap_in[1])
            self.line("b2")
            arrive(self.blk(2, z, y, x), self.swap_in[2])
            self.line("c2")

        def fans(self, name, zz):
            k, yy, xx, _ = self.columns[name]
            b = self.blk(k, zz, yy, xx)
            if k == 0:
                return [push(b, b, x_peer, self.fan_a, self.via[0] + zz, start=False),
                        push(b, b, y_peer, self.fan_a, self.via[1] + zz, start=False)]
            return [push(b, b, y_peer if k == 1 else x_peer, self.fan_bc, self.full[k], start=False)]

        def share(self, *names):
            for name in names:
                for c in self.fans(name, z):
                    c.start()

        def step(self, s, *names):
            for name in names:
                k, yy, xx, base = self.columns[name]
                for cond, zz, go, nxt in ways[s]:
                    b = self.blk(k, zz, yy, xx)
                    relay = push(b, b, nxt, self.line_out[k], base + zz, start=False)
                    fans = self.fans(name, zz)

                    def act():
                        relay.wait_recv()
                        if s < nz - 2:
                            pl.when(go)(relay.start)
                        for c in fans:
                            c.start()

                    pl.when(cond)(act)

        def third(self, s):
            lo, span = self.sets[0]
            for cond, zz in [(None, z)] if s < 0 else [(w[0], w[1]) for w in ways[s]]:
                full = self.blk(0, zz, y, x)
                b = x_all.at[g, self.kind, at(zz, y, 1 - x), :, pl.ds(lo, span // 2)]
                tx = push(b, b, y_peer, self.fan_a, self.full[0], start=False)
                b = x_all.at[g, self.kind, at(zz, 1 - y, x), :, pl.ds(lo + span // 2, span // 2)]
                ty = push(b, b, x_peer, self.fan_a, self.full[0], start=False)

                def act():
                    arrive(full, self.via[0] + zz)
                    tx.start()
                    arrive(full, self.via[1] + zz)
                    ty.start()

                when(cond, act)

        def land(self, k):
            arrive(self.some(k, nz if k == 0 else 2 * nz), self.full[k])

    late = []

    def lone(src, dst, gg):
        k = next(send_slots)
        owed.append((None, src, k))
        return push(src, dst, me, k, next(recv_slots), gg)

    def spread(kind):
        for d in range(1, groups):
            late.append(lone(x_all.at[g, kind], x_all.at[g, kind], (g + d) % groups))

    def lines():
        g1.lines1()
        g1.lines2()

    def share():
        g1.share("a", "b1", "c1", "b2", "c2")

    g0, g1 = Gather(0), Gather(1)
    g0.register()
    g1.register()
    g0.swap()
    g0.lines1()
    g0.share("a", "b1", "c1")
    g0.lines2()
    g0.share("b2", "c2")
    loads[1].wait()
    g1.swap()
    for s in range(nz - 2):
        g0.step(s, "a")
        g0.third(s - 1)
        g0.step(s, "b1", "c1", "b2", "c2")
    g0.step(nz - 2, "a")
    g0.third(nz - 3)
    g0.step(nz - 2, "b1", "c1")
    g0.third(nz - 2)
    g0.step(nz - 2, "b2", "c2")
    g0.owe()
    lines()
    share()

    offset = me * shard
    step = 256
    loads[4].wait()
    top = jnp.full((1, tokens), -jnp.inf, F32)
    for k in range(3):
        g0.land(k)
        lo, span = sets[k]
        h = x_all[g, 0, :, :, lo:lo + span].reshape(tokens, span)
        for i in range(0, shard, step):
            lg = lax.dot_general(table[i:i + step, lo:lo + span], h, (((1,), (1,)), ((), ())),
                                 preferred_element_type=F32)
            if k > 0:
                lg = lg + logits[i:i + step]
            if k == 2:
                top = jnp.maximum(top, jnp.max(lg, axis=0, keepdims=True))
            logits[i:i + step] = lg
    loads[3].wait()
    total = jnp.zeros((1, tokens), F32)
    pick = jnp.zeros((1, tokens), F32)
    tgt = tgt_ref[...]
    for i in range(0, shard, step):
        lg = logits[i:i + step]
        vocab_row = offset + i + lax.broadcasted_iota(jnp.int32, (step, tokens), 0)
        total = total + jnp.sum(jnp.exp(lg - top), axis=0, keepdims=True)
        pick = pick + jnp.sum(jnp.where(vocab_row == tgt, lg, 0.0), axis=0, keepdims=True)
    line = lax.broadcasted_iota(jnp.int32, (4, tokens), 0)
    mine = jnp.where(line == 0, top, jnp.where(line == 1, total, pick))
    st[pl.ds(me, 1)] = mine[None]
    stat_out, stat_in = next(send_slots), next(recv_slots)
    for d in range(1, n):
        push(st.at[me], st.at[me], (me + d) % n, stat_out, stat_in)
    owed.append((None, st.at[pl.ds(0, n - 1)], stat_out))

    g1.step(0, "a")
    g1.third(-1)
    g1.step(0, "b1", "c1", "b2", "c2")
    spread(0)
    loads[2].wait()
    for d in range(1, groups):
        late.append(lone(ids.at[0], ids.at[groups - d], (g + d) % groups))
    for s in range(1, nz - 2):
        g1.step(s, "a")
        g1.third(s - 1)
        g1.step(s, "b1", "c1", "b2", "c2")
    arrive(st.at[pl.ds(0, n - 1)], stat_in)
    top = st[0, 0:1]
    for j in range(1, n):
        top = jnp.maximum(top, st[j, 0:1])
    total = jnp.zeros((1, tokens), F32)
    pick = jnp.zeros((1, tokens), F32)
    for j in range(n):
        total = total + st[j, 1:2] * jnp.exp(st[j, 0:1] - top)
        pick = pick + st[j, 2:3]
    lse = top + jnp.log(total)
    loss_ref[...] = lse - pick
    for i in range(0, shard, step):
        vocab_row = offset + i + lax.broadcasted_iota(jnp.int32, (step, tokens), 0)
        hit = (vocab_row == tgt).astype(F32)
        d = (jnp.exp(logits[i:i + step] - lse) - hit).astype(BF16)
        dl_ref[i:i + step] = d
        dlt_ref[:, i:i + step] = d.T

    chunks = chunk_list(half)
    outs = [next(send_slots) for _ in range(3)]
    owed.extend([(None, s1, outs[0]), (None, s2, outs[1]), (None, s3, outs[2])])
    ins = {(stage, side, c): next(recv_slots) for stage in range(3) for side in range(2) for c in range(len(chunks))}

    def send_first(c):
        lo, wide = chunks[c]
        for side in range(2):
            base = side * half + lo
            p = jnp.dot(dlt_ref[...], table[:, base:base + wide], preferred_element_type=F32)
            part[:, :, :, :, base:base + wide] = p.reshape(nz, 2, 2, rows, wide)
            if side == 0:
                p = part[:, pl.ds(1 - y, 1), :, :, base:base + wide]
            else:
                p = part[:, :, pl.ds(1 - x, 1), :, base:base + wide]
            s1[side, :, :, :, lo:lo + wide] = p.reshape(nz, 2, rows, wide).astype(BF16)
            cols = pl.ds(lo, wide)
            push(s1.at[side, :, :, :, cols], r1.at[side, :, :, :, cols],
                 y_peer if side == 0 else x_peer, outs[0], ins[0, side, c])

    def merged_first(side, c, zz, yy, xx, count):
        lo, wide = chunks[c]
        base = side * half + lo
        a = part[pl.ds(zz, count), pl.ds(yy, 1), pl.ds(xx, 1), :, base:base + wide].reshape(count, rows, wide)
        b = r1[side, pl.ds(zz, count), pl.ds(xx if side == 0 else yy, 1), :, lo:lo + wide].reshape(count, rows, wide)
        return a + b.astype(F32)

    def send_second(c):
        lo, wide = chunks[c]
        for side in range(2):
            arrive(r1.at[side, :, :, :, pl.ds(lo, wide)], ins[0, side, c])
            yy, xx, peer = (y, 1 - x, x_peer) if side == 0 else (1 - y, x, y_peer)
            s2[side, :, :, lo:lo + wide] = merged_first(side, c, 0, yy, xx, nz).astype(BF16)
            cols = pl.ds(lo, wide)
            push(s2.at[side, :, :, cols], r2.at[side, :, :, cols], peer, outs[1], ins[1, side, c])

    def merged(side, c, zz):
        lo, wide = chunks[c]
        return (merged_first(side, c, zz, y, x, 1)
                + r2[side, pl.ds(zz, 1), :, lo:lo + wide].astype(F32)).reshape(rows, wide)

    def send_last(c):
        lo, wide = chunks[c]
        for side in range(2):
            arrive(r2.at[side, :, :, pl.ds(lo, wide)], ins[1, side, c])
            for d in range(1, nz):
                zz = (z + d) % nz
                s3[side, d - 1, :, lo:lo + wide] = merged(side, c, zz).astype(BF16)
                cols = pl.ds(lo, wide)
                push(s3.at[side, d - 1, :, cols], r3.at[side, d - 1, :, cols], at(zz, y, x), outs[2], ins[2, side, c])

    def tail(c):
        lo, wide = chunks[c]
        for side in range(2):
            arrive(r3.at[side, :, :, pl.ds(lo, wide)], ins[2, side, c])
            acc = merged(side, c, z)
            for d in range(1, nz):
                acc = acc + r3[side, d - 1, :, lo:lo + wide].astype(F32)
            base = side * half + lo
            hg_ref[:, base:base + wide] = acc.astype(BF16)

    def send_dl():
        for d in range(1, groups):
            peer = (g + d) % groups
            late.append(lone(dl_ref.at[pl.ds(pl.multiple_of(peer * piece, piece), piece)],
                             e_in.at[groups - d - 1], peer))

    def build_hot():
        line = me * shard + g * piece + lax.broadcasted_iota(jnp.int32, (piece, tokens), 0)
        for d in range(groups):
            hot[d] = (line == ids[d]).astype(F32).astype(BF16)

    def settle():
        for c in late:
            c.wait_recv()
        late.clear()

    def grad(t, kind):
        cols = slice(t * TILE, (t + 1) * TILE)
        acc = None
        for d in range(groups):
            if kind == 1:
                e = hot[d]
            elif d == 0:
                e = dl_ref[pl.ds(pl.multiple_of(g * piece, piece), piece)]
            else:
                e = e_in[d - 1]
            p = jnp.dot(e, x_all[(g + d) % groups, kind, :, :, cols].reshape(tokens, TILE),
                        preferred_element_type=F32)
            acc = p if acc is None else acc + p
        if kind == 1:
            acc = acc + tg_ref[:, cols]
        tg_ref[:, cols] = acc

    tiles = width // TILE
    send_first(0)
    send_dl()
    g1.step(nz - 2, "a", "b1", "c1", "b2", "c2")
    send_first(1)
    settle()
    build_hot()
    for t in range(tiles):
        grad(t, 0)
    send_second(0)
    send_first(2)
    g1.third(nz - 3)
    g1.third(nz - 2)
    g1.owe()
    send_second(1)
    send_last(0)
    send_first(3)
    for k in range(3):
        g1.land(k)
    spread(1)
    send_second(2)
    send_last(1)
    send_second(3)
    send_last(2)
    send_last(3)
    settle()
    for t in range(tiles):
        grad(t, 1)
    drain()
    for c in range(len(chunks)):
        tail(c)


def write_kernel(tg_ref, hg_ref, loss_ref, tg_out, hg_out, loss_out, sem):
    width = tg_ref.shape[1]
    parts = tg_ref.shape[0] // 64
    copies = [pltpu.make_async_copy(hg_ref, hg_out, sem.at[0]), pltpu.make_async_copy(loss_ref, loss_out, sem.at[1])]
    for i in range(parts):
        r = pl.ds(i * 64, 64)
        copies.append(pltpu.make_async_copy(tg_ref.at[r], tg_out.at[r], sem.at[2 + i]))
    for c in copies:
        c.start()
    for c in copies:
        c.wait()


def solution(mesh):
    groups, n = mesh.shape["dp"], mesh.shape["vocab"]

    def body(table, hidden, cotangent, input_ids, target_ids):
        rows, width = hidden.shape
        shard = table.shape[0]
        nz = n // 4
        tokens = n * rows
        half = width // 2
        piece = shard // groups
        sends, recvs = count_semaphores(groups, n, len(chunk_list(half)))
        anys = pl.BlockSpec(memory_space=pl.ANY)
        vmem = pl.BlockSpec(memory_space=pltpu.VMEM)
        buffers = [
            pltpu.VMEM((shard, width), BF16),
            pltpu.VMEM((groups, 2, n, rows, width), BF16),
            pltpu.VMEM((shard, tokens), F32),
            pltpu.VMEM((n, 4, tokens), F32),
            pltpu.VMEM((shard, tokens), BF16),
            pltpu.VMEM((tokens, shard), BF16),
            pltpu.VMEM((groups - 1, piece, tokens), BF16),
            pltpu.VMEM((groups, piece, tokens), BF16),
            pltpu.VMEM((groups, 1, tokens), jnp.int32),
            pltpu.VMEM((1, tokens), jnp.int32),
            pltpu.VMEM((nz, 2, 2, rows, width), F32),
            pltpu.VMEM((2, nz, 2, rows, half), BF16),
            pltpu.VMEM((2, nz, 2, rows, half), BF16),
            pltpu.VMEM((2, nz, rows, half), BF16),
            pltpu.VMEM((2, nz, rows, half), BF16),
            pltpu.VMEM((2, nz - 1, rows, half), BF16),
            pltpu.VMEM((2, nz - 1, rows, half), BF16),
        ]
        used = sum(math.prod(b.shape) * jnp.dtype(b.dtype).itemsize for b in buffers)
        tg, hg, loss = pl.pallas_call(
            functools.partial(kernel, groups, n),
            out_shape=(
                pltpu.VMEM((piece, width), F32),
                pltpu.VMEM((rows, width), BF16),
                pltpu.VMEM((1, tokens), F32),
            ),
            in_specs=[anys] * 5,
            out_specs=(vmem, vmem, vmem),
            scratch_shapes=buffers + [
                pltpu.SemaphoreType.DMA((5,)),
                pltpu.SemaphoreType.DMA((sends,)),
                pltpu.SemaphoreType.DMA((recvs,)),
            ],
            compiler_params=pltpu.CompilerParams(
                collective_id=0, has_side_effects=True, vmem_limit_bytes=used + 6 * 2**20),
        )(*(pltpu.with_memory_space_constraint(a, pltpu.HBM) for a in (
            table, hidden, cotangent, input_ids.reshape(1, tokens), target_ids.reshape(1, tokens))))
        tg = pltpu.with_memory_space_constraint(tg, pltpu.VMEM)
        hg = pltpu.with_memory_space_constraint(hg, pltpu.VMEM)
        loss = pltpu.with_memory_space_constraint(loss, pltpu.VMEM)
        table_grad, hg, loss = pl.pallas_call(
            write_kernel,
            out_shape=(
                jax.ShapeDtypeStruct((piece, width), F32),
                jax.ShapeDtypeStruct((rows, width), BF16),
                jax.ShapeDtypeStruct((1, tokens), F32),
            ),
            in_specs=[vmem] * 3,
            out_specs=(anys,) * 3,
            scratch_shapes=[pltpu.SemaphoreType.DMA((2 + piece // 64,))],
            compiler_params=pltpu.CompilerParams(vmem_limit_bytes=2 * 2**20),
        )(tg, hg, loss)
        return table_grad, hg, loss.reshape(tokens)

    return jax.shard_map(
        body,
        mesh=mesh,
        in_specs=(
            P("vocab", None),
            P(("dp", "vocab"), None),
            P(("dp", "vocab"), None),
            P("dp"),
            P("dp"),
        ),
        out_specs=(P(("vocab", "dp"), None), P(("dp", "vocab"), None), P("dp")),
        check_vma=False,
    )
```

```python
import functools
import math

import jax
import jax.numpy as jnp
from jax import lax
from jax.experimental import pallas as pl
from jax.experimental.pallas import tpu as pltpu
from jax.sharding import PartitionSpec as P

MESH = pl.DeviceIdType.MESH
BF16 = jnp.bfloat16
F32 = jnp.float32
TILE = 512
HIDDEN_A = 6
COT_A = 6


def chunk_list(half):
    eighth = half // 8
    spans, lo = [], 0
    for k in (2, 3, 2, 1):
        spans.append((lo, k * eighth))
        lo += k * eighth
    return spans


def count_semaphores(groups, n, chunks):
    nz = n // 4
    gather = 2 + 5 * (nz - 1) + 2 * nz + 3
    return 12 + 1 + 3 + 4 * (groups - 1), 2 * gather + 1 + 5 * chunks + 4 * (groups - 1)


def kernel(groups, n, table_hbm, hidden_hbm, cot_hbm, in_ids_hbm, tgt_hbm,
           tg_ref, hg_ref, loss_ref,
           table, x_all, logits, st, dl_ref, dlt_ref, e_in, hot, ids, tgt_ref,
           part, s1, r1, s2, r2, s3, r3, load_sem, send, recv):
    nz = n // 4
    rows, width = hg_ref.shape
    shard = table.shape[0]
    tokens = n * rows
    piece = shard // groups
    half = width // 2
    me = lax.axis_index("vocab")
    g = lax.axis_index("dp")
    z = me // 4
    y = (me % 4) // 2
    x = me % 2
    send_slots, recv_slots = iter(range(send.shape[0])), iter(range(recv.shape[0]))

    def at(zz, yy, xx):
        return zz * 4 + yy * 2 + xx

    x_peer = at(z, y, 1 - x)
    y_peer = at(z, 1 - y, x)
    above, below = z + 1 < nz, z > 0
    up, down = at(jnp.minimum(z + 1, nz - 1), y, x), at(jnp.maximum(z - 1, 0), y, x)

    def when(cond, act):
        if cond is None:
            act()
        else:
            pl.when(cond)(act)

    def every(cond, acts):
        def act():
            for one in acts:
                one()
        when(cond, act)

    barrier = pltpu.get_barrier_semaphore()

    def greet(v, gg=None):
        pl.semaphore_signal(barrier, inc=1, device_id=(g if gg is None else gg, v), device_id_type=MESH)

    greet(x_peer)
    greet(y_peer)
    when(above, lambda: greet(up))
    when(below, lambda: greet(down))
    for d in range(1, groups):
        greet(me, (g + d) % groups)

    loads = [
        pltpu.make_async_copy(hidden_hbm, x_all.at[g, 0, me], load_sem.at[0]),
        pltpu.make_async_copy(cot_hbm, x_all.at[g, 1, me], load_sem.at[1]),
        pltpu.make_async_copy(in_ids_hbm, ids.at[0], load_sem.at[2]),
        pltpu.make_async_copy(tgt_hbm, tgt_ref, load_sem.at[3]),
        pltpu.make_async_copy(table_hbm, table, load_sem.at[4]),
    ]
    for c in loads:
        c.start()
    loads[0].wait()
    pl.semaphore_wait(barrier, 2 + above.astype(jnp.int32) + below.astype(jnp.int32) + groups - 1)

    owed = []

    def push(src, dst, v, out, into, gg=None, cond=None, start=True):
        c = pltpu.make_async_remote_copy(
            src_ref=src, dst_ref=dst, send_sem=send.at[out], recv_sem=recv.at[into],
            device_id=(g if gg is None else gg, v), device_id_type=MESH)
        if start:
            when(cond, c.start)
        return c

    def drain():
        for cond, ref, out in owed:
            c = pltpu.make_async_remote_copy(
                src_ref=ref, dst_ref=ref, send_sem=send.at[out], recv_sem=recv.at[0],
                device_id=(g, me), device_id_type=MESH)
            when(cond, c.wait_send)
        owed.clear()

    def arrive(ref, into):
        pltpu.make_async_remote_copy(
            src_ref=ref, dst_ref=ref, send_sem=send.at[0], recv_sem=recv.at[into],
            device_id=(g, me), device_id_type=MESH).wait_recv()

    def take(it, count):
        return [next(it) for _ in range(count)][0]

    def split(k):
        wa = width * k // 16
        wb = (width - wa) // 2
        return [(0, wa), (wa, wb), (wa + wb, wb)]

    both = [split(HIDDEN_A), split(COT_A)]
    sets = both[0]
    inner = jnp.logical_and(above, below)
    outer = jnp.logical_not(inner)
    ways = []
    for s in range(nz - 1):
        lower, upper = z - 1 - s >= 0, z + 1 + s < nz
        ways.append(((lower, jnp.maximum(z - 1 - s, 0), above, up), (upper, jnp.minimum(z + 1 + s, nz - 1), below, down)))

    class Gather:
        def __init__(self, kind):
            self.kind, self.sets = kind, both[kind]
            self.swap_out, self.fan_a, self.fan_bc = (next(send_slots) for _ in range(3))
            self.line_out = [next(send_slots) for _ in range(3)]
            self.swap_in = [None, next(recv_slots), next(recv_slots)]
            self.full = [next(recv_slots) for _ in range(3)]
            self.via = {0: take(recv_slots, nz), 1: take(recv_slots, nz)}

            def some(k, count):
                return x_all.at[g, kind, pl.ds(0, count), :, pl.ds(*self.sets[k])]

            self.some = some
            self.columns = {}

        def owe(self):
            owed.append((None, self.some(1, 1), self.swap_out))
            owed.append((None, self.some(2, 1), self.swap_out))
            owed.append((None, self.some(0, 3 * nz), self.fan_a))
            owed.append((None, self.some(1, 2 * nz), self.fan_bc))
            owed.append((None, self.some(2, 2 * nz), self.fan_bc))
            for k in range(3):
                lines = 1 if k == 0 else 2
                owed.append((inner, self.some(k, lines * (nz + 1)), self.line_out[k]))
                owed.append((outer, self.some(k, lines), self.line_out[k]))

        def blk(self, k, zz, yy, xx):
            return x_all.at[g, self.kind, at(zz, yy, xx), :, pl.ds(*self.sets[k])]

        def swap(self):
            for k, peer in ((1, x_peer), (2, y_peer)):
                b = self.blk(k, z, y, x)
                push(b, b, peer, self.swap_out, self.swap_in[k])

        def register(self):
            for name, k, yy, xx in (("a", 0, y, x), ("b1", 1, y, x), ("c1", 2, y, x),
                                    ("b2", 1, y, 1 - x), ("c2", 2, 1 - y, x)):
                self.columns[name] = (k, yy, xx, take(recv_slots, nz - 1))

        def line(self, name):
            k, yy, xx, base = self.columns[name]
            b = self.blk(k, z, yy, xx)
            push(b, b, up, self.line_out[k], base + jnp.minimum(z, nz - 2), cond=above)
            push(b, b, down, self.line_out[k], base + jnp.maximum(z - 1, 0), cond=below)

        def lines1(self):
            self.line("a")
            self.line("b1")
            self.line("c1")

        def lines2(self):
            arrive(self.blk(1, z, y, x), self.swap_in[1])
            self.line("b2")
            arrive(self.blk(2, z, y, x), self.swap_in[2])
            self.line("c2")

        def fans(self, name, zz):
            k, yy, xx, _ = self.columns[name]
            b = self.blk(k, zz, yy, xx)
            if k == 0:
                return [push(b, b, x_peer, self.fan_a, self.via[0] + zz, start=False),
                        push(b, b, y_peer, self.fan_a, self.via[1] + zz, start=False)]
            return [push(b, b, y_peer if k == 1 else x_peer, self.fan_bc, self.full[k], start=False)]

        def share(self, *names):
            for name in names:
                for c in self.fans(name, z):
                    c.start()

        def step(self, s, *names):
            for name in names:
                k, yy, xx, base = self.columns[name]
                for cond, zz, go, nxt in ways[s]:
                    slot = base + (zz if nxt is up else zz - 1)
                    b = self.blk(k, zz, yy, xx)
                    relay = push(b, b, nxt, self.line_out[k], slot, start=False)
                    fans = self.fans(name, zz)

                    def act():
                        relay.wait_recv()
                        if s < nz - 2:
                            pl.when(go)(relay.start)
                        for c in fans:
                            c.start()

                    pl.when(cond)(act)

        def third(self, s):
            lo, span = self.sets[0]
            for cond, zz in [(None, z)] if s < 0 else [(w[0], w[1]) for w in ways[s]]:
                full = self.blk(0, zz, y, x)
                b = x_all.at[g, self.kind, at(zz, y, 1 - x), :, pl.ds(lo, span // 2)]
                tx = push(b, b, y_peer, self.fan_a, self.full[0], start=False)
                b = x_all.at[g, self.kind, at(zz, 1 - y, x), :, pl.ds(lo + span // 2, span // 2)]
                ty = push(b, b, x_peer, self.fan_a, self.full[0], start=False)

                def act():
                    arrive(full, self.via[0] + zz)
                    tx.start()
                    arrive(full, self.via[1] + zz)
                    ty.start()

                when(cond, act)

        def land(self, k):
            arrive(self.some(k, nz if k == 0 else 2 * nz), self.full[k])

    late = []

    def lone(src, dst, gg):
        k = next(send_slots)
        owed.append((None, src, k))
        return push(src, dst, me, k, next(recv_slots), gg)

    def spread(kind):
        for d in range(1, groups):
            late.append(lone(x_all.at[g, kind], x_all.at[g, kind], (g + d) % groups))

    def lines():
        g1.lines1()
        g1.lines2()

    def share():
        g1.share("a", "b1", "c1", "b2", "c2")

    g0, g1 = Gather(0), Gather(1)
    g0.register()
    g1.register()
    g0.swap()
    g0.lines1()
    g0.share("a", "b1", "c1")
    g0.lines2()
    g0.share("b2", "c2")
    loads[1].wait()
    g1.swap()
    for s in range(nz - 2):
        g0.step(s, "a")
        g0.third(s - 1)
        g0.step(s, "b1", "c1", "b2", "c2")
    g0.step(nz - 2, "a")
    g0.third(nz - 3)
    g0.step(nz - 2, "b1", "c1")
    g0.third(nz - 2)
    g0.step(nz - 2, "b2", "c2")
    g0.owe()
    lines()
    share()

    offset = me * shard
    step = 256
    loads[4].wait()
    top = jnp.full((1, tokens), -jnp.inf, F32)
    for k in range(3):
        g0.land(k)
        lo, span = sets[k]
        h = x_all[g, 0, :, :, lo:lo + span].reshape(tokens, span)
        for i in range(0, shard, step):
            lg = lax.dot_general(table[i:i + step, lo:lo + span], h, (((1,), (1,)), ((), ())),
                                 preferred_element_type=F32)
            if k > 0:
                lg = lg + logits[i:i + step]
            if k == 2:
                top = jnp.maximum(top, jnp.max(lg, axis=0, keepdims=True))
            logits[i:i + step] = lg
    loads[3].wait()
    total = jnp.zeros((1, tokens), F32)
    pick = jnp.zeros((1, tokens), F32)
    tgt = tgt_ref[...]
    for i in range(0, shard, step):
        lg = logits[i:i + step]
        vocab_row = offset + i + lax.broadcasted_iota(jnp.int32, (step, tokens), 0)
        total = total + jnp.sum(jnp.exp(lg - top), axis=0, keepdims=True)
        pick = pick + jnp.sum(jnp.where(vocab_row == tgt, lg, 0.0), axis=0, keepdims=True)
    line = lax.broadcasted_iota(jnp.int32, (4, tokens), 0)
    mine = jnp.where(line == 0, top, jnp.where(line == 1, total, pick))
    st[pl.ds(me, 1)] = mine[None]
    stat_out, stat_in = next(send_slots), next(recv_slots)
    for d in range(1, n):
        push(st.at[me], st.at[me], (me + d) % n, stat_out, stat_in)
    owed.append((None, st.at[pl.ds(0, n - 1)], stat_out))

    g1.step(0, "a")
    g1.third(-1)
    g1.step(0, "b1", "c1", "b2", "c2")
    spread(0)
    loads[2].wait()
    for d in range(1, groups):
        late.append(lone(ids.at[0], ids.at[groups - d], (g + d) % groups))
    for s in range(1, nz - 2):
        g1.step(s, "a")
        g1.third(s - 1)
        g1.step(s, "b1", "c1", "b2", "c2")
    arrive(st.at[pl.ds(0, n - 1)], stat_in)
    top = st[0, 0:1]
    for j in range(1, n):
        top = jnp.maximum(top, st[j, 0:1])
    total = jnp.zeros((1, tokens), F32)
    pick = jnp.zeros((1, tokens), F32)
    for j in range(n):
        total = total + st[j, 1:2] * jnp.exp(st[j, 0:1] - top)
        pick = pick + st[j, 2:3]
    lse = top + jnp.log(total)
    loss_ref[...] = lse - pick
    for i in range(0, shard, step):
        vocab_row = offset + i + lax.broadcasted_iota(jnp.int32, (step, tokens), 0)
        hit = (vocab_row == tgt).astype(F32)
        d = (jnp.exp(logits[i:i + step] - lse) - hit).astype(BF16)
        dl_ref[i:i + step] = d
        dlt_ref[:, i:i + step] = d.T

    chunks = chunk_list(half)
    outs = [next(send_slots) for _ in range(3)]
    owed.extend([(None, s1, outs[0]), (None, s2, outs[1]), (None, s3, outs[2])])
    ins = {(stage, side, c): next(recv_slots) for stage in range(2) for side in range(2) for c in range(len(chunks))}
    ends = [next(recv_slots) for _ in chunks]

    def send_first(c):
        lo, wide = chunks[c]
        for side in range(2):
            base = side * half + lo
            p = jnp.dot(dlt_ref[...], table[:, base:base + wide], preferred_element_type=F32)
            part[:, :, :, :, base:base + wide] = p.reshape(nz, 2, 2, rows, wide)
            if side == 0:
                p = part[:, pl.ds(1 - y, 1), :, :, base:base + wide]
            else:
                p = part[:, :, pl.ds(1 - x, 1), :, base:base + wide]
            s1[side, :, :, :, lo:lo + wide] = p.reshape(nz, 2, rows, wide).astype(BF16)
            cols = pl.ds(lo, wide)
            push(s1.at[side, :, :, :, cols], r1.at[side, :, :, :, cols],
                 y_peer if side == 0 else x_peer, outs[0], ins[0, side, c])

    def merged_first(side, c, zz, yy, xx, count):
        lo, wide = chunks[c]
        base = side * half + lo
        a = part[pl.ds(zz, count), pl.ds(yy, 1), pl.ds(xx, 1), :, base:base + wide].reshape(count, rows, wide)
        b = r1[side, pl.ds(zz, count), pl.ds(xx if side == 0 else yy, 1), :, lo:lo + wide].reshape(count, rows, wide)
        return a + b.astype(F32)

    def send_second(c):
        lo, wide = chunks[c]
        for side in range(2):
            arrive(r1.at[side, :, :, :, pl.ds(lo, wide)], ins[0, side, c])
            yy, xx, peer = (y, 1 - x, x_peer) if side == 0 else (1 - y, x, y_peer)
            s2[side, :, :, lo:lo + wide] = merged_first(side, c, 0, yy, xx, nz).astype(BF16)
            cols = pl.ds(lo, wide)
            push(s2.at[side, :, :, cols], r2.at[side, :, :, cols], peer, outs[1], ins[1, side, c])

    def merged(side, c, zz):
        lo, wide = chunks[c]
        return (merged_first(side, c, zz, y, x, 1)
                + r2[side, pl.ds(zz, 1), :, lo:lo + wide].astype(F32)).reshape(rows, wide)

    def send_last(c):
        lo, wide = chunks[c]
        for side in range(2):
            arrive(r2.at[side, :, :, pl.ds(lo, wide)], ins[1, side, c])
            for d in range(1, nz):
                zz = (z + d) % nz
                s3[side, d - 1, :, lo:lo + wide] = merged(side, c, zz).astype(BF16)
                cols = pl.ds(lo, wide)
                push(s3.at[side, d - 1, :, cols], r3.at[side, d - 1, :, cols], at(zz, y, x), outs[2], ends[c])

    def tail(c):
        lo, wide = chunks[c]
        arrive(r3.at[:, :, :, pl.ds(lo, wide)], ends[c])
        for side in range(2):
            acc = merged(side, c, z)
            for d in range(1, nz):
                acc = acc + r3[side, d - 1, :, lo:lo + wide].astype(F32)
            base = side * half + lo
            hg_ref[:, base:base + wide] = acc.astype(BF16)

    def send_dl():
        for d in range(1, groups):
            peer = (g + d) % groups
            late.append(lone(dl_ref.at[pl.ds(pl.multiple_of(peer * piece, piece), piece)],
                             e_in.at[groups - d - 1], peer))

    def build_hot():
        line = me * shard + g * piece + lax.broadcasted_iota(jnp.int32, (piece, tokens), 0)
        for d in range(groups):
            hot[d] = (line == ids[d]).astype(F32).astype(BF16)

    def settle():
        for c in late:
            c.wait_recv()
        late.clear()

    def grad(t, kind):
        cols = slice(t * TILE, (t + 1) * TILE)
        acc = None
        for d in range(groups):
            if kind == 1:
                e = hot[d]
            elif d == 0:
                e = dl_ref[pl.ds(pl.multiple_of(g * piece, piece), piece)]
            else:
                e = e_in[d - 1]
            p = jnp.dot(e, x_all[(g + d) % groups, kind, :, :, cols].reshape(tokens, TILE),
                        preferred_element_type=F32)
            acc = p if acc is None else acc + p
        if kind == 1:
            acc = acc + tg_ref[:, cols]
        tg_ref[:, cols] = acc

    tiles = width // TILE
    send_first(0)
    send_dl()
    g1.step(nz - 2, "a", "b1", "c1", "b2", "c2")
    send_first(1)
    settle()
    build_hot()
    for t in range(tiles):
        grad(t, 0)
    send_second(0)
    send_first(2)
    g1.third(nz - 3)
    g1.third(nz - 2)
    g1.owe()
    send_second(1)
    send_last(0)
    send_first(3)
    for k in range(3):
        g1.land(k)
    spread(1)
    send_second(2)
    send_last(1)
    send_second(3)
    send_last(2)
    send_last(3)
    settle()
    for t in range(tiles):
        grad(t, 1)
    drain()
    for c in range(len(chunks)):
        tail(c)


def write_kernel(tg_ref, hg_ref, loss_ref, tg_out, hg_out, loss_out, sem):
    width = tg_ref.shape[1]
    parts = tg_ref.shape[0] // 64
    copies = [pltpu.make_async_copy(hg_ref, hg_out, sem.at[0]), pltpu.make_async_copy(loss_ref, loss_out, sem.at[1])]
    for i in range(parts):
        r = pl.ds(i * 64, 64)
        copies.append(pltpu.make_async_copy(tg_ref.at[r], tg_out.at[r], sem.at[2 + i]))
    for c in copies:
        c.start()
    for c in copies:
        c.wait()


def solution(mesh):
    groups, n = mesh.shape["dp"], mesh.shape["vocab"]

    def body(table, hidden, cotangent, input_ids, target_ids):
        rows, width = hidden.shape
        shard = table.shape[0]
        nz = n // 4
        tokens = n * rows
        half = width // 2
        piece = shard // groups
        sends, recvs = count_semaphores(groups, n, len(chunk_list(half)))
        anys = pl.BlockSpec(memory_space=pl.ANY)
        vmem = pl.BlockSpec(memory_space=pltpu.VMEM)
        buffers = [
            pltpu.VMEM((shard, width), BF16),
            pltpu.VMEM((groups, 2, n, rows, width), BF16),
            pltpu.VMEM((shard, tokens), F32),
            pltpu.VMEM((n, 4, tokens), F32),
            pltpu.VMEM((shard, tokens), BF16),
            pltpu.VMEM((tokens, shard), BF16),
            pltpu.VMEM((groups - 1, piece, tokens), BF16),
            pltpu.VMEM((groups, piece, tokens), BF16),
            pltpu.VMEM((groups, 1, tokens), jnp.int32),
            pltpu.VMEM((1, tokens), jnp.int32),
            pltpu.VMEM((nz, 2, 2, rows, width), F32),
            pltpu.VMEM((2, nz, 2, rows, half), BF16),
            pltpu.VMEM((2, nz, 2, rows, half), BF16),
            pltpu.VMEM((2, nz, rows, half), BF16),
            pltpu.VMEM((2, nz, rows, half), BF16),
            pltpu.VMEM((2, nz - 1, rows, half), BF16),
            pltpu.VMEM((2, nz - 1, rows, half), BF16),
        ]
        used = sum(math.prod(b.shape) * jnp.dtype(b.dtype).itemsize for b in buffers)
        tg, hg, loss = pl.pallas_call(
            functools.partial(kernel, groups, n),
            out_shape=(
                pltpu.VMEM((piece, width), F32),
                pltpu.VMEM((rows, width), BF16),
                pltpu.VMEM((1, tokens), F32),
            ),
            in_specs=[anys] * 5,
            out_specs=(vmem, vmem, vmem),
            scratch_shapes=buffers + [
                pltpu.SemaphoreType.DMA((5,)),
                pltpu.SemaphoreType.DMA((sends,)),
                pltpu.SemaphoreType.DMA((recvs,)),
            ],
            compiler_params=pltpu.CompilerParams(
                collective_id=0, has_side_effects=True, vmem_limit_bytes=used + 6 * 2**20),
        )(*(pltpu.with_memory_space_constraint(a, pltpu.HBM) for a in (
            table, hidden, cotangent, input_ids.reshape(1, tokens), target_ids.reshape(1, tokens))))
        tg = pltpu.with_memory_space_constraint(tg, pltpu.VMEM)
        hg = pltpu.with_memory_space_constraint(hg, pltpu.VMEM)
        loss = pltpu.with_memory_space_constraint(loss, pltpu.VMEM)
        table_grad, hg, loss = pl.pallas_call(
            write_kernel,
            out_shape=(
                jax.ShapeDtypeStruct((piece, width), F32),
                jax.ShapeDtypeStruct((rows, width), BF16),
                jax.ShapeDtypeStruct((1, tokens), F32),
            ),
            in_specs=[vmem] * 3,
            out_specs=(anys,) * 3,
            scratch_shapes=[pltpu.SemaphoreType.DMA((2 + piece // 64,))],
            compiler_params=pltpu.CompilerParams(vmem_limit_bytes=2 * 2**20),
        )(tg, hg, loss)
        return table_grad, hg, loss.reshape(tokens)

    return jax.shard_map(
        body,
        mesh=mesh,
        in_specs=(
            P("vocab", None),
            P(("dp", "vocab"), None),
            P(("dp", "vocab"), None),
            P("dp"),
            P("dp"),
        ),
        out_specs=(P(("vocab", "dp"), None), P(("dp", "vocab"), None), P("dp")),
        check_vma=False,
    )
```
